32 devices in a mesh: row: 2 (over x), col: 16 (over z, y, core).
Axes of the slice: x: 2, y: 2, z: 4, core: 2. Of those that a mesh axis runs over, the one named last changes fastest.
Arguments:
- matrix: bfloat16 [768, 262144], P('row', 'col'), may hold values from -0.01171875 to 0.01171875
- probes: bfloat16 [262144, 128], P('col'), may hold values from -6 to 6
Outputs:
- krylov: bfloat16 [2, 262144, 128], P(None, 'col')
The draws below stay inside these ranges and needn't reach their ends.
All inputs are finite; a program needn't handle non-finite values.
Results may differ from the reference program's by a relative error of at most 0.0054.
Values may be sent and summed in bfloat16 or wider, within the bound.
A program may use at most 128 MiB of HBM per device.

```python
import math
import jax
import jax.numpy as jnp
from jax import lax

N = 262144
K = 128
ITERS = 2
M = 768


def level_of(own_key, extent, split, smallest, largest):
    gain, own = 1.0, jax.random.fold_in(own_key, 6)
    for axis_at, shards_of in split:
        draws = jnp.exp(jax.random.uniform(jax.random.fold_in(own, axis_at), (shards_of,), jnp.float32, smallest / len(split), largest / len(split)))
        gain = gain * jnp.repeat(draws, extent[axis_at] // shards_of).reshape([-1 if axis == axis_at else 1 for axis in range(len(extent))])
    return gain


def bell_draw(own_key, extent, scale, limit, pieces=(), kind=jnp.bfloat16):
    result = jax.random.normal(own_key, extent, jnp.float32) * scale
    if len(pieces) > 0:
        result = level_of(own_key, extent, pieces, -0.22, 0.18) * result
    return jnp.clip(result, min=-limit, max=limit).astype(kind)


def setup_inputs(seed: int = 0) -> dict:
    streams_of = jax.random.split(jax.random.key(seed), 3)
    return {
        "matrix": bell_draw(streams_of[0], (M, N), N ** -0.5, 0.01171875, ((0, 2), (1, 16))),
        "probes": bell_draw(streams_of[1], (N, K), 1.0, 6.0, ((0, 16),)),
    }


def reference(matrix, probes):
    stretch = math.sqrt(N / M)
    current = probes
    results = []
    for level in range(ITERS):
        factor = 1.0 if level == 0 else 1.0 / stretch
        partial_value = jnp.dot(matrix, current, preferred_element_type=jnp.float32)
        reduced = (partial_value * factor).astype(jnp.bfloat16)
        back = lax.dot_general(matrix, reduced, (((0,), (0,)), ((), ())), preferred_element_type=jnp.float32)
        current = (back * stretch).astype(jnp.bfloat16)
        results.append(current)
    return jnp.stack(results)
```

```python
import functools
import math

import jax
import jax.numpy as jnp
from jax import lax
from jax.experimental import pallas as pl
from jax.experimental.pallas import tpu as pltpu
from jax.sharding import PartitionSpec as P

ITERS = 2
HALVES = 2
CHUNK = 1024
TILE = 1024
SPARE = 1024
MESH = pl.DeviceIdType.MESH


def plain_body(matrix, probes):
    m_total = matrix.shape[0] * lax.axis_size("row")
    n_total = matrix.shape[1] * lax.axis_size("col")
    stretch = math.sqrt(n_total / m_total)
    current = probes
    results = []
    for level in range(ITERS):
        factor = 1.0 if level == 0 else 1.0 / stretch
        partial_value = jnp.dot(matrix, current, preferred_element_type=jnp.float32)
        summed = lax.psum(partial_value, "col")
        reduced = (summed * factor).astype(jnp.bfloat16)
        whole_term = lax.dot_general(
            matrix, reduced, (((0,), (0,)), ((), ())), preferred_element_type=jnp.float32
        )
        portion = lax.psum_scatter(whole_term, "row", scatter_dimension=0, tiled=True)
        current = lax.all_gather(
            (portion * stretch).astype(jnp.bfloat16), "row", axis=0, tiled=True
        )
        results.append(current)
    return jnp.stack(results)


def kernel(
    stretch, cols, chunk, tile, spare,
    a_hbm, x_hbm, out,
    a, x, own, got, total, part, slot, zrow, zall, ztall, far, zcross, zfar, zallfar,
    a_sem, x_sem, psend, precv, rsend, rrecv, gsend, grecv,
    fsend, frecv, zsend, zrecv, hsend, hrecv,
):
    rows, width = a.shape
    k = x.shape[1]
    kh = k // HALVES
    main = width - spare
    steps = main // tile
    chunks = width // chunk
    share = rows // cols
    mine = lax.axis_index("col")
    other = 1 - lax.axis_index("row")

    def load(i):
        return pl.ds(pl.multiple_of(i * chunk, chunk), chunk)

    def span(i):
        return pl.ds(pl.multiple_of(i * tile, tile), tile)

    rest = pl.ds(main, spare)

    def a_copy(i):
        return pltpu.make_async_copy(a_hbm.at[:, load(i)], a.at[:, load(i)], a_sem.at[i])

    def x_copy(i):
        return pltpu.make_async_copy(x_hbm.at[load(i)], x.at[load(i)], x_sem.at[i])

    def swap(level, half, i):
        return pltpu.make_async_remote_copy(
            src_ref=own.at[level, half, i], dst_ref=got.at[level, half, i],
            send_sem=psend.at[level, half], recv_sem=precv.at[level, half, i],
            device_id={"row": other}, device_id_type=MESH,
        )

    def swaps(level, half):
        return pltpu.make_async_remote_copy(
            src_ref=own.at[level, half], dst_ref=got.at[level, half],
            send_sem=psend.at[level, half], recv_sem=precv.at[level, half, 0],
            device_id={"row": other}, device_id_type=MESH,
        )

    def each(buffer, stage, send_sem, recv_sem):
        peers = buffer.at[stage, pl.ds(1, cols - 1)]
        return pltpu.make_async_remote_copy(
            src_ref=peers, dst_ref=peers,
            send_sem=send_sem.at[stage], recv_sem=recv_sem.at[stage],
            device_id={"col": lax.rem(mine + 1, cols)}, device_id_type=MESH,
        )

    def piece(i):
        return pl.ds(pl.multiple_of(i * share, share), share)

    def scatter(stage, off):
        peer = lax.rem(mine + off, cols)
        return pltpu.make_async_remote_copy(
            src_ref=part.at[stage, piece(peer)], dst_ref=slot.at[stage, off],
            send_sem=rsend.at[stage], recv_sem=rrecv.at[stage],
            device_id={"col": peer}, device_id_type=MESH,
        )

    def spread(stage, off):
        peer = lax.rem(mine + off, cols)
        return pltpu.make_async_remote_copy(
            src_ref=zrow.at[stage], dst_ref=zall.at[stage, off],
            send_sem=gsend.at[stage], recv_sem=grecv.at[stage],
            device_id={"col": peer}, device_id_type=MESH,
        )

    def far_copy():
        return pltpu.make_async_remote_copy(
            src_ref=a_hbm.at[:, rest], dst_ref=far,
            send_sem=fsend, recv_sem=frecv,
            device_id={"row": other}, device_id_type=MESH,
        )

    def cross(level):
        return pltpu.make_async_remote_copy(
            src_ref=zcross.at[level], dst_ref=zfar.at[level],
            send_sem=zsend.at[level], recv_sem=zrecv.at[level],
            device_id={"row": other}, device_id_type=MESH,
        )

    def spread_far(level, off):
        peer = lax.rem(mine + off, cols)
        return pltpu.make_async_remote_copy(
            src_ref=zfar.at[level], dst_ref=zallfar.at[level, off],
            send_sem=hsend.at[level], recv_sem=hrecv.at[level],
            device_id={"col": peer}, device_id_type=MESH,
        )

    @pl.loop(0, chunks)
    def _(i):
        a_copy(i).start()
        x_copy(i).start()

    barrier = pltpu.get_barrier_semaphore()
    pl.semaphore_signal(barrier, inc=1, device_id={"row": other}, device_id_type=MESH)

    @pl.loop(1, cols)
    def _(off):
        pl.semaphore_signal(
            barrier, inc=1, device_id={"col": lax.rem(mine + off, cols)}, device_id_type=MESH
        )

    pl.semaphore_wait(barrier, cols)

    far_copy().start()

    part[0] = jnp.zeros((rows, k), jnp.float32)

    @pl.loop(0, chunks)
    def _(i):
        a_copy(i).wait()
        x_copy(i).wait()
        part[0] += jnp.dot(a[:, load(i)], x[load(i)], preferred_element_type=jnp.float32)

    def gather(into, own_rows, level, send_sem, recv_sem):
        each(into, level, send_sem, recv_sem).wait_recv()
        total[piece(mine)] = own_rows.astype(jnp.float32)

        @pl.loop(1, cols)
        def _(off):
            source = lax.rem(mine + cols - off, cols)
            total[piece(source)] = into[level, off].astype(jnp.float32)

        return total[...].T.astype(jnp.bfloat16)

    def reduce(stage, factor):
        @pl.loop(1, cols)
        def _(off):
            scatter(stage, off).start()

        each(slot, stage, rsend, rrecv).wait_recv()
        acc = part[stage, piece(mine)]
        for off in range(1, cols):
            acc += slot[stage, off]
        zrow[stage] = (acc * factor).astype(jnp.bfloat16)

        @pl.loop(1, cols)
        def _(off):
            spread(stage, off).start()

    def send(level, half, stage):
        lines = slice(half * kh, (half + 1) * kh)

        @pl.loop(0, steps)
        def _(i):
            term = jnp.dot(
                ztall[stage, lines], a[:, span(i)], preferred_element_type=jnp.float32
            )
            own[level, half, i] = (term * stretch).astype(jnp.bfloat16)
            swap(level, half, i).start()

    def joined(level, half, i):
        swap(level, half, i).wait_recv()
        both = own[level, half, i].astype(jnp.float32) + got[level, half, i].astype(jnp.float32)
        return both.astype(jnp.bfloat16)

    def padded(y, half):
        blank = jnp.zeros_like(y)
        return jnp.concatenate([y, blank] if half == 0 else [blank, y], axis=0)

    def project(where, y):
        return lax.dot_general(
            a[:, where], y, (((1,), (1,)), ((), ())), preferred_element_type=jnp.float32
        )

    def upright(y):
        return y.astype(jnp.float32).T.astype(jnp.bfloat16)

    def near_far(level, stages):
        cross(level).wait_recv()

        @pl.loop(1, cols)
        def _(off):
            spread_far(level, off).start()

        z_far = gather(zallfar, zfar[level], level, hsend, hrecv)
        z = jnp.concatenate(
            [ztall[s, h * kh:(h + 1) * kh] for h, s in enumerate(stages)], axis=0
        )
        near_term = jnp.dot(z, a[:, rest], preferred_element_type=jnp.float32)
        far_term = jnp.dot(z_far, far[...], preferred_element_type=jnp.float32)
        y = ((near_term + far_term) * stretch).astype(jnp.bfloat16)
        out[level, rest] = upright(y)
        return y

    reduce(0, 1.0)
    zcross[0] = zrow[0]
    cross(0).start()
    ztall[0] = gather(zall, zrow[0], 0, gsend, grecv)
    send(0, 0, 0)
    send(0, 1, 0)

    far_copy().wait_recv()
    y_rest = near_far(0, (0, 0))
    part[1] = project(rest, padded(y_rest[:kh], 0))
    part[2] = project(rest, padded(y_rest[kh:], 1))

    @pl.loop(0, steps)
    def _(i):
        y = joined(0, 0, i)
        got[0, 0, i] = y
        part[1] += project(span(i), padded(y, 0))

    reduce(1, 1.0 / stretch)
    ztall[1] = gather(zall, zrow[1], 1, gsend, grecv)
    send(1, 0, 1)

    @pl.loop(0, steps)
    def _(i):
        y = joined(0, 1, i)
        part[2] += project(span(i), padded(y, 1))
        out[0, span(i)] = upright(jnp.concatenate([got[0, 0, i], y], axis=0))

    reduce(2, 1.0 / stretch)
    zcross[1] = zrow[1] + zrow[2]
    cross(1).start()
    ztall[2] = gather(zall, zrow[2], 2, gsend, grecv)
    send(1, 1, 2)

    @pl.loop(0, steps)
    def _(i):
        got[1, 0, i] = joined(1, 0, i)

    near_far(1, (1, 2))

    @pl.loop(0, steps)
    def _(i):
        y = joined(1, 1, i)
        out[1, span(i)] = upright(jnp.concatenate([got[1, 0, i], y], axis=0))

    far_copy().wait_send()

    for stage in range(ITERS + 1):
        each(slot, stage, rsend, rrecv).wait_send()
        each(zall, stage, gsend, grecv).wait_send()

    for level in range(ITERS):
        each(zallfar, level, hsend, hrecv).wait_send()
        cross(level).wait_send()
        for half in range(HALVES):
            swaps(level, half).wait_send()


def paired_body(matrix, probes):
    rows, width = matrix.shape
    k = probes.shape[1]
    kh = k // HALVES
    cols = lax.axis_size("col")
    stretch = math.sqrt(width * cols / (rows * lax.axis_size("row")))
    chunk = CHUNK
    tile = TILE
    spare = SPARE
    steps = (width - spare) // tile
    share = rows // cols
    stages = ITERS + 1
    dma = pltpu.SemaphoreType.DMA
    return pl.pallas_call(
        functools.partial(kernel, stretch, cols, chunk, tile, spare),
        out_shape=pltpu.VMEM((ITERS, width, k), jnp.bfloat16),
        in_specs=[pl.BlockSpec(memory_space=pl.ANY)] * 2,
        out_specs=pl.BlockSpec(memory_space=pltpu.VMEM),
        scratch_shapes=[
            pltpu.VMEM((rows, width), jnp.bfloat16),
            pltpu.VMEM((width, k), jnp.bfloat16),
            pltpu.VMEM((ITERS, HALVES, steps, kh, tile), jnp.bfloat16),
            pltpu.VMEM((ITERS, HALVES, steps, kh, tile), jnp.bfloat16),
            pltpu.VMEM((rows, k), jnp.float32),
            pltpu.VMEM((stages, rows, k), jnp.float32),
            pltpu.VMEM((stages, cols, share, k), jnp.float32),
            pltpu.VMEM((stages, share, k), jnp.bfloat16),
            pltpu.VMEM((stages, cols, share, k), jnp.bfloat16),
            pltpu.VMEM((stages, k, rows), jnp.bfloat16),
            pltpu.VMEM((rows, spare), jnp.bfloat16),
            pltpu.VMEM((ITERS, share, k), jnp.bfloat16),
            pltpu.VMEM((ITERS, share, k), jnp.bfloat16),
            pltpu.VMEM((ITERS, cols, share, k), jnp.bfloat16),
            dma((width // chunk,)),
            dma((width // chunk,)),
            dma((ITERS, HALVES)),
            dma((ITERS, HALVES, steps)),
            dma((stages,)),
            dma((stages,)),
            dma((stages,)),
            dma((stages,)),
            dma,
            dma,
            dma((ITERS,)),
            dma((ITERS,)),
            dma((ITERS,)),
            dma((ITERS,)),
        ],
        compiler_params=pltpu.CompilerParams(
            vmem_limit_bytes=46 * 2**20, collective_id=0, has_side_effects=True
        ),
    )(matrix, probes)


def solution(mesh):
    placed = (P("row", "col"), P("col", None))
    body = paired_body if mesh.shape["row"] == 2 else plain_body
    return jax.shard_map(
        body, mesh=mesh, in_specs=placed, out_specs=P(None, "col", None), check_vma=False
    )
```

```python
import functools
import math

import jax
import jax.numpy as jnp
from jax import lax
from jax.experimental import pallas as pl
from jax.experimental.pallas import tpu as pltpu
from jax.sharding import PartitionSpec as P

ITERS = 2
HALVES = 2
CHUNK = 2048
TILE = 1024
SPARE = 1152
MESH = pl.DeviceIdType.MESH


def plain_body(matrix, probes):
    m_total = matrix.shape[0] * lax.axis_size("row")
    n_total = matrix.shape[1] * lax.axis_size("col")
    stretch = math.sqrt(n_total / m_total)
    current = probes
    results = []
    for level in range(ITERS):
        factor = 1.0 if level == 0 else 1.0 / stretch
        partial_value = jnp.dot(matrix, current, preferred_element_type=jnp.float32)
        summed = lax.psum(partial_value, "col")
        reduced = (summed * factor).astype(jnp.bfloat16)
        whole_term = lax.dot_general(
            matrix, reduced, (((0,), (0,)), ((), ())), preferred_element_type=jnp.float32
        )
        portion = lax.psum_scatter(whole_term, "row", scatter_dimension=0, tiled=True)
        current = lax.all_gather(
            (portion * stretch).astype(jnp.bfloat16), "row", axis=0, tiled=True
        )
        results.append(current)
    return jnp.stack(results)


def kernel(
    stretch, cols, chunk, tile, spare,
    a_hbm, x_hbm, out,
    a, x, own, got, own_last, got_last, total, part, slot, zrow, zall, ztall, far, zcross, zfar, zallfar,
    a_sem, x_sem, psend, precv, rsend, rrecv, gsend, grecv,
    fsend, frecv, zsend, zrecv, hsend, hrecv,
):
    rows, width = a.shape
    k = x.shape[1]
    kh = k // HALVES
    main = width - spare
    steps = (main - 1) // tile
    last = main - steps * tile
    chunks = width // chunk
    share = rows // cols
    mine = lax.axis_index("col")
    other = 1 - lax.axis_index("row")

    def load(i):
        return pl.ds(pl.multiple_of(i * chunk, chunk), chunk)

    def span(i):
        if i is None:
            return pl.ds(steps * tile, last)
        return pl.ds(pl.multiple_of(i * tile, tile), tile)

    def sent(level, half, i):
        return own_last.at[level, half] if i is None else own.at[level, half, i]

    def landed(level, half, i):
        return got_last.at[level, half] if i is None else got.at[level, half, i]

    def tiles(body):
        pl.loop(0, steps)(body)
        body(None)

    rest = pl.ds(main, spare)

    def a_copy(i):
        return pltpu.make_async_copy(a_hbm.at[:, load(i)], a.at[:, load(i)], a_sem.at[i])

    def x_copy(i):
        return pltpu.make_async_copy(x_hbm.at[load(i)], x.at[load(i)], x_sem.at[i])

    def swap(level, half, i):
        return pltpu.make_async_remote_copy(
            src_ref=sent(level, half, i), dst_ref=landed(level, half, i),
            send_sem=psend.at[level, half, 0 if i is not None else 1],
            recv_sem=precv.at[level, half, steps if i is None else i],
            device_id={"row": other}, device_id_type=MESH,
        )

    def swaps(level, half):
        return pltpu.make_async_remote_copy(
            src_ref=own.at[level, half], dst_ref=got.at[level, half],
            send_sem=psend.at[level, half, 0], recv_sem=precv.at[level, half, 0],
            device_id={"row": other}, device_id_type=MESH,
        )

    def each(buffer, stage, send_sem, recv_sem):
        peers = buffer.at[stage, pl.ds(1, cols - 1)]
        return pltpu.make_async_remote_copy(
            src_ref=peers, dst_ref=peers,
            send_sem=send_sem.at[stage], recv_sem=recv_sem.at[stage],
            device_id={"col": lax.rem(mine + 1, cols)}, device_id_type=MESH,
        )

    def partner(code):
        if cols & (cols - 1):
            return lax.rem(mine + code, cols)
        peer, bit = 0, 1
        while bit < cols:
            digit = lax.rem(mine // bit, 2)
            peer += bit * (1 - digit if code & bit else digit)
            bit *= 2
        return peer

    def sender(code):
        return lax.rem(mine + cols - code, cols) if cols & (cols - 1) else partner(code)

    codes = range(cols - 1, 0, -1)

    def piece(i):
        return pl.ds(pl.multiple_of(i * share, share), share)

    def scatter(stage, off):
        peer = partner(off)
        return pltpu.make_async_remote_copy(
            src_ref=part.at[stage, piece(peer)], dst_ref=slot.at[stage, off],
            send_sem=rsend.at[stage], recv_sem=rrecv.at[stage],
            device_id={"col": peer}, device_id_type=MESH,
        )

    def spread(stage, off):
        peer = partner(off)
        return pltpu.make_async_remote_copy(
            src_ref=zrow.at[stage], dst_ref=zall.at[stage, off],
            send_sem=gsend.at[stage], recv_sem=grecv.at[stage],
            device_id={"col": peer}, device_id_type=MESH,
        )

    def far_copy():
        return pltpu.make_async_remote_copy(
            src_ref=a_hbm.at[:, rest], dst_ref=far,
            send_sem=fsend, recv_sem=frecv,
            device_id={"row": other}, device_id_type=MESH,
        )

    def cross(level):
        return pltpu.make_async_remote_copy(
            src_ref=zcross.at[level], dst_ref=zfar.at[level],
            send_sem=zsend.at[level], recv_sem=zrecv.at[level],
            device_id={"row": other}, device_id_type=MESH,
        )

    def spread_far(level, off):
        peer = partner(off)
        return pltpu.make_async_remote_copy(
            src_ref=zfar.at[level], dst_ref=zallfar.at[level, off],
            send_sem=hsend.at[level], recv_sem=hrecv.at[level],
            device_id={"col": peer}, device_id_type=MESH,
        )

    @pl.loop(0, chunks)
    def _(i):
        a_copy(i).start()
        x_copy(i).start()

    barrier = pltpu.get_barrier_semaphore()
    leader = 3 * cols // 4 - 1
    pl.semaphore_signal(barrier, inc=1, device_id={"row": other}, device_id_type=MESH)

    @pl.when(mine != leader)
    def _():
        pl.semaphore_wait(barrier, 1)
        far_copy().start()
        pl.semaphore_signal(barrier, inc=1, device_id={"col": leader}, device_id_type=MESH)

    part[0] = jnp.zeros((rows, k), jnp.float32)

    def first_product(i):
        a_copy(i).wait()
        x_copy(i).wait()
        part[0] += jnp.dot(a[:, load(i)], x[load(i)], preferred_element_type=jnp.float32)

    pl.loop(0, chunks // 4)(first_product)

    @pl.when(mine == leader)
    def _():
        pl.semaphore_wait(barrier, cols)
        far_copy().start()

        @pl.loop(1, cols)
        def _(off):
            pl.semaphore_signal(
                barrier, inc=1, device_id={"col": lax.rem(mine + off, cols)}, device_id_type=MESH
            )

    pl.loop(chunks // 4, chunks)(first_product)

    @pl.when(mine != leader)
    def _():
        pl.semaphore_wait(barrier, 1)

    def gather(into, own_rows, level, send_sem, recv_sem):
        each(into, level, send_sem, recv_sem).wait_recv()
        total[piece(mine)] = own_rows.astype(jnp.float32)
        for off in codes:
            total[piece(sender(off))] = into[level, off].astype(jnp.float32)
        return total[...].T.astype(jnp.bfloat16)

    def reduce(stage, factor):
        for off in codes:
            scatter(stage, off).start()
        each(slot, stage, rsend, rrecv).wait_recv()
        acc = part[stage, piece(mine)]
        for off in codes:
            acc += slot[stage, off]
        zrow[stage] = (acc * factor).astype(jnp.bfloat16)
        for off in codes:
            spread(stage, off).start()

    def send(level, half, stage):
        lines = slice(half * kh, (half + 1) * kh)

        @tiles
        def _(i):
            term = jnp.dot(
                ztall[stage, lines], a[:, span(i)], preferred_element_type=jnp.float32
            )
            sent(level, half, i)[...] = (term * stretch).astype(jnp.bfloat16)
            swap(level, half, i).start()

    def joined(level, half, i):
        swap(level, half, i).wait_recv()
        near = sent(level, half, i)[...].astype(jnp.float32)
        both = near + landed(level, half, i)[...].astype(jnp.float32)
        return both.astype(jnp.bfloat16)

    def padded(y, half):
        blank = jnp.zeros_like(y)
        return jnp.concatenate([y, blank] if half == 0 else [blank, y], axis=0)

    def project(where, y):
        return lax.dot_general(
            a[:, where], y, (((1,), (1,)), ((), ())), preferred_element_type=jnp.float32
        )

    def upright(y):
        return y.astype(jnp.float32).T.astype(jnp.bfloat16)

    def near_far(level, stages):
        cross(level).wait_recv()

        for off in codes:
            spread_far(level, off).start()

        z_far = gather(zallfar, zfar[level], level, hsend, hrecv)
        z = jnp.concatenate(
            [ztall[s, h * kh:(h + 1) * kh] for h, s in enumerate(stages)], axis=0
        )
        near_term = jnp.dot(z, a[:, rest], preferred_element_type=jnp.float32)
        far_term = jnp.dot(z_far, far[...], preferred_element_type=jnp.float32)
        y = ((near_term + far_term) * stretch).astype(jnp.bfloat16)
        out[level, rest] = upright(y)
        return y

    reduce(0, 1.0)
    zcross[0] = zrow[0]
    cross(0).start()
    ztall[0] = gather(zall, zrow[0], 0, gsend, grecv)
    send(0, 0, 0)
    send(0, 1, 0)

    far_copy().wait_recv()
    y_rest = near_far(0, (0, 0))
    part[1] = project(rest, padded(y_rest[:kh], 0))
    part[2] = project(rest, padded(y_rest[kh:], 1))

    @tiles
    def _(i):
        y = joined(0, 0, i)
        landed(0, 0, i)[...] = y
        part[1] += project(span(i), padded(y, 0))

    reduce(1, 1.0 / stretch)
    ztall[1] = gather(zall, zrow[1], 1, gsend, grecv)
    send(1, 0, 1)

    @tiles
    def _(i):
        y = joined(0, 1, i)
        part[2] += project(span(i), padded(y, 1))
        out[0, span(i)] = upright(jnp.concatenate([landed(0, 0, i)[...], y], axis=0))

    reduce(2, 1.0 / stretch)
    zcross[1] = zrow[1] + zrow[2]
    cross(1).start()
    ztall[2] = gather(zall, zrow[2], 2, gsend, grecv)
    send(1, 1, 2)

    @tiles
    def _(i):
        landed(1, 0, i)[...] = joined(1, 0, i)

    near_far(1, (1, 2))

    @tiles
    def _(i):
        y = joined(1, 1, i)
        out[1, span(i)] = upright(jnp.concatenate([landed(1, 0, i)[...], y], axis=0))

    far_copy().wait_send()

    for stage in range(ITERS + 1):
        each(slot, stage, rsend, rrecv).wait_send()
        each(zall, stage, gsend, grecv).wait_send()

    for level in range(ITERS):
        each(zallfar, level, hsend, hrecv).wait_send()
        cross(level).wait_send()
        for half in range(HALVES):
            swaps(level, half).wait_send()
            swap(level, half, None).wait_send()


def paired_body(matrix, probes):
    rows, width = matrix.shape
    k = probes.shape[1]
    kh = k // HALVES
    cols = lax.axis_size("col")
    stretch = math.sqrt(width * cols / (rows * lax.axis_size("row")))
    chunk = CHUNK
    tile = TILE
    spare = SPARE
    steps = (width - spare - 1) // tile
    last = width - spare - steps * tile
    share = rows // cols
    stages = ITERS + 1
    dma = pltpu.SemaphoreType.DMA
    return pl.pallas_call(
        functools.partial(kernel, stretch, cols, chunk, tile, spare),
        out_shape=pltpu.VMEM((ITERS, width, k), jnp.bfloat16),
        in_specs=[pl.BlockSpec(memory_space=pl.ANY)] * 2,
        out_specs=pl.BlockSpec(memory_space=pltpu.VMEM),
        scratch_shapes=[
            pltpu.VMEM((rows, width), jnp.bfloat16),
            pltpu.VMEM((width, k), jnp.bfloat16),
            pltpu.VMEM((ITERS, HALVES, steps, kh, tile), jnp.bfloat16),
            pltpu.VMEM((ITERS, HALVES, steps, kh, tile), jnp.bfloat16),
            pltpu.VMEM((ITERS, HALVES, kh, last), jnp.bfloat16),
            pltpu.VMEM((ITERS, HALVES, kh, last), jnp.bfloat16),
            pltpu.VMEM((rows, k), jnp.float32),
            pltpu.VMEM((stages, rows, k), jnp.float32),
            pltpu.VMEM((stages, cols, share, k), jnp.float32),
            pltpu.VMEM((stages, share, k), jnp.bfloat16),
            pltpu.VMEM((stages, cols, share, k), jnp.bfloat16),
            pltpu.VMEM((stages, k, rows), jnp.bfloat16),
            pltpu.VMEM((rows, spare), jnp.bfloat16),
            pltpu.VMEM((ITERS, share, k), jnp.bfloat16),
            pltpu.VMEM((ITERS, share, k), jnp.bfloat16),
            pltpu.VMEM((ITERS, cols, share, k), jnp.bfloat16),
            dma((width // chunk,)),
            dma((width // chunk,)),
            dma((ITERS, HALVES, 2)),
            dma((ITERS, HALVES, steps + 1)),
            dma((stages,)),
            dma((stages,)),
            dma((stages,)),
            dma((stages,)),
            dma,
            dma,
            dma((ITERS,)),
            dma((ITERS,)),
            dma((ITERS,)),
            dma((ITERS,)),
        ],
        compiler_params=pltpu.CompilerParams(
            vmem_limit_bytes=46 * 2**20, collective_id=0, has_side_effects=True
        ),
    )(matrix, probes)


def solution(mesh):
    placed = (P("row", "col"), P("col", None))
    body = paired_body if mesh.shape["row"] == 2 else plain_body
    return jax.shard_map(
        body, mesh=mesh, in_specs=placed, out_specs=P(None, "col", None), check_vma=False
    )
```

```python
import functools
import math

import jax
import jax.numpy as jnp
from jax import lax
from jax.experimental import pallas as pl
from jax.experimental.pallas import tpu as pltpu
from jax.sharding import PartitionSpec as P

ITERS = 2
HALVES = 2
CHUNK = 2048
LINES = 8
WIDER = 4
GROUP = 7
TILE = 1024
SPARE = 1024
MESH = pl.DeviceIdType.MESH


def plain_body(matrix, probes):
    m_total = matrix.shape[0] * lax.axis_size("row")
    n_total = matrix.shape[1] * lax.axis_size("col")
    stretch = math.sqrt(n_total / m_total)
    current = probes
    results = []
    for level in range(ITERS):
        factor = 1.0 if level == 0 else 1.0 / stretch
        partial_value = jnp.dot(matrix, current, preferred_element_type=jnp.float32)
        summed = lax.psum(partial_value, "col")
        reduced = (summed * factor).astype(jnp.bfloat16)
        whole_term = lax.dot_general(
            matrix, reduced, (((0,), (0,)), ((), ())), preferred_element_type=jnp.float32
        )
        portion = lax.psum_scatter(whole_term, "row", scatter_dimension=0, tiled=True)
        current = lax.all_gather(
            (portion * stretch).astype(jnp.bfloat16), "row", axis=0, tiled=True
        )
        results.append(current)
    return jnp.stack(results)


def kernel(
    stretch, cols, chunk, tile, spare,
    a_hbm, x_hbm, out,
    a, x, own, got, own_last, got_last, part, slot, zrow, zall, ztall, far, zcross, zfar, zallfar,
    a_sem, x_sem, psend, precv, rsend, rrecv, gsend, grecv,
    fsend, frecv, zsend, zrecv, hsend, hrecv,
):
    rows, width = a.shape
    k = x.shape[1]
    kh = k // HALVES
    main = width - spare
    steps = (main - 1) // tile
    last = main - steps * tile
    group = math.gcd(steps, GROUP)
    groups = steps // group
    share = rows // cols
    blocks = share // LINES
    band = rows // blocks
    mine = lax.axis_index("col")
    other = 1 - lax.axis_index("row")

    def cut(block):
        return chunk if block == 0 else WIDER * chunk

    def load(block, i):
        return pl.ds(pl.multiple_of(i * cut(block), cut(block)), cut(block))

    def lines(block):
        return pl.ds(block * band, band)

    def span(i):
        if i is None:
            return pl.ds(steps * tile, last)
        return pl.ds(pl.multiple_of(i * tile, tile), tile)

    def sent(level, half, i):
        return own_last.at[level, half] if i is None else own.at[level, half, i]

    def landed(level, half, i):
        return got_last.at[level, half] if i is None else got.at[level, half, i]

    def tiles(body):
        pl.loop(0, steps)(body)
        body(None)

    def arrivals(level, half):
        def run(body):
            @pl.loop(0, groups)
            def _(g):
                arrival(level, half, g).wait_recv()
                pl.loop(g * group, (g + 1) * group)(body)

            swap(level, half, None).wait_recv()
            body(None)

        return run

    rest = pl.ds(main, spare)

    def a_copy(block, i):
        where = (lines(block), load(block, i))
        first = 0 if block == 0 else width // chunk + (block - 1) * (width // cut(1))
        return pltpu.make_async_copy(a_hbm.at[where], a.at[where], a_sem.at[first + i])

    def x_copy(i):
        where = load(0, i)
        return pltpu.make_async_copy(x_hbm.at[where], x.at[where], x_sem.at[i])

    def swap(level, half, i):
        return pltpu.make_async_remote_copy(
            src_ref=sent(level, half, i), dst_ref=landed(level, half, i),
            send_sem=psend.at[0 if i is not None else 1],
            recv_sem=precv.at[level, half, groups if i is None else i // group],
            device_id={"row": other}, device_id_type=MESH,
        )

    def arrival(level, half, g):
        members = (level, half, pl.ds(g * group, group))
        return pltpu.make_async_remote_copy(
            src_ref=own.at[members], dst_ref=got.at[members],
            send_sem=psend.at[0], recv_sem=precv.at[level, half, g],
            device_id={"row": other}, device_id_type=MESH,
        )

    def departure(i):
        return pltpu.make_async_remote_copy(
            src_ref=(own, own_last)[i], dst_ref=(got, got_last)[i],
            send_sem=psend.at[i], recv_sem=precv.at[0, 0, 0],
            device_id={"row": other}, device_id_type=MESH,
        )

    def each(buffer, where, send_sem, recv_sem):
        peers = buffer.at[(*where, pl.ds(1, cols - 1))]
        return pltpu.make_async_remote_copy(
            src_ref=peers, dst_ref=peers,
            send_sem=send_sem.at[where[0]], recv_sem=recv_sem.at[where],
            device_id={"col": lax.rem(mine + 1, cols)}, device_id_type=MESH,
        )

    def partner(code):
        if cols & (cols - 1):
            return lax.rem(mine + code, cols)
        peer, bit = 0, 1
        while bit < cols:
            digit = lax.rem(mine // bit, 2)
            peer += bit * (1 - digit if code & bit else digit)
            bit *= 2
        return peer

    codes = range(cols - 1, 0, -1)

    def piece(block, i):
        return pl.ds(pl.multiple_of(block * band + i * LINES, LINES), LINES)

    def scatter(stage, block, code):
        peer = partner(code)
        return pltpu.make_async_remote_copy(
            src_ref=part.at[stage, piece(block, peer)], dst_ref=slot.at[stage, block, code],
            send_sem=rsend.at[stage], recv_sem=rrecv.at[stage, block],
            device_id={"col": peer}, device_id_type=MESH,
        )

    def spread(stage, block, code):
        return pltpu.make_async_remote_copy(
            src_ref=zrow.at[stage, block], dst_ref=zall.at[stage, block, mine],
            send_sem=gsend.at[stage], recv_sem=grecv.at[stage, block],
            device_id={"col": partner(code)}, device_id_type=MESH,
        )

    def far_copy():
        return pltpu.make_async_remote_copy(
            src_ref=a_hbm.at[:, rest], dst_ref=far,
            send_sem=fsend, recv_sem=frecv,
            device_id={"row": other}, device_id_type=MESH,
        )

    def cross(level):
        return pltpu.make_async_remote_copy(
            src_ref=zcross.at[level], dst_ref=zfar.at[level],
            send_sem=zsend.at[level], recv_sem=zrecv.at[level],
            device_id={"row": other}, device_id_type=MESH,
        )

    def spread_far(level, code):
        return pltpu.make_async_remote_copy(
            src_ref=zfar.at[level], dst_ref=zallfar.at[level, mine],
            send_sem=hsend.at[level], recv_sem=hrecv.at[level],
            device_id={"col": partner(code)}, device_id_type=MESH,
        )

    for block in range(blocks):

        @pl.loop(0, width // cut(block))
        def _(i):
            if block == 0:
                x_copy(i).start()
            a_copy(block, i).start()

    barrier = pltpu.get_barrier_semaphore()
    leader = 3 * cols // 4 - 1
    pl.semaphore_signal(barrier, inc=1, device_id={"row": other}, device_id_type=MESH)

    @pl.when(mine != leader)
    def _():
        pl.semaphore_wait(barrier, 1)
        far_copy().start()
        pl.semaphore_signal(barrier, inc=1, device_id={"col": leader}, device_id_type=MESH)

    part[0] = jnp.zeros((rows, k), jnp.float32)

    def first_product(block):
        def step(i):
            if block == 0:
                x_copy(i).wait()
            a_copy(block, i).wait()
            where = load(block, i)
            part[0, lines(block)] += jnp.dot(
                a[lines(block), where], x[where], preferred_element_type=jnp.float32
            )

        return step

    def scatters(stage, block):
        for code in codes:
            scatter(stage, block, code).start()

    def settle(stage, block, factor):
        each(slot, (stage, block), rsend, rrecv).wait_recv()
        acc = part[stage, piece(block, mine)]
        for code in codes:
            acc += slot[stage, block, code]
        zrow[stage, block] = (acc * factor).astype(jnp.bfloat16)
        for code in codes:
            spread(stage, block, code).start()

    def across(pieces):
        return pieces.astype(jnp.float32).reshape(band, k).T.astype(jnp.bfloat16)

    def gather(stage):
        for block in range(blocks):
            each(zall, (stage, block), gsend, grecv).wait_recv()
            zall[stage, block, mine] = zrow[stage, block]
            ztall[stage, :, lines(block)] = across(zall[stage, block])

    def reduce(stage, factor):
        for block in range(blocks):
            scatters(stage, block)
        for block in range(blocks):
            settle(stage, block, factor)

    half_way = width // chunk // 2
    pl.loop(0, half_way)(first_product(0))

    @pl.when(mine == leader)
    def _():
        pl.semaphore_wait(barrier, cols)
        far_copy().start()

        @pl.loop(1, cols)
        def _(off):
            pl.semaphore_signal(
                barrier, inc=1, device_id={"col": lax.rem(mine + off, cols)}, device_id_type=MESH
            )

    pl.loop(half_way, width // chunk)(first_product(0))

    @pl.when(mine != leader)
    def _():
        pl.semaphore_wait(barrier, 1)

    scatters(0, 0)
    for block in range(1, blocks):
        pl.loop(0, width // cut(block))(first_product(block))
        scatters(0, block)

    def send(level, half, stage):
        kept = slice(half * kh, (half + 1) * kh)

        @tiles
        def _(i):
            term = jnp.dot(
                ztall[stage, kept], a[:, span(i)], preferred_element_type=jnp.float32
            )
            sent(level, half, i)[...] = (term * stretch).astype(jnp.bfloat16)
            swap(level, half, i).start()

    def joined(level, half, i):
        near = sent(level, half, i)[...].astype(jnp.float32)
        both = near + landed(level, half, i)[...].astype(jnp.float32)
        return both.astype(jnp.bfloat16)

    def padded(y, half):
        blank = jnp.zeros_like(y)
        return jnp.concatenate([y, blank] if half == 0 else [blank, y], axis=0)

    def project(where, y):
        return lax.dot_general(
            a[:, where], y, (((1,), (1,)), ((), ())), preferred_element_type=jnp.float32
        )

    def upright(y):
        return y.astype(jnp.float32).T.astype(jnp.bfloat16)

    def near_far(level, stages):
        cross(level).wait_recv()

        for off in codes:
            spread_far(level, off).start()

        each(zallfar, (level,), hsend, hrecv).wait_recv()
        zallfar[level, mine] = zfar[level]
        z_far = jnp.concatenate(
            [across(zallfar[level, :, block]) for block in range(blocks)], axis=1
        )
        z = jnp.concatenate(
            [ztall[s, h * kh:(h + 1) * kh] for h, s in enumerate(stages)], axis=0
        )
        near_term = jnp.dot(z, a[:, rest], preferred_element_type=jnp.float32)
        far_term = jnp.dot(z_far, far[...], preferred_element_type=jnp.float32)
        y = ((near_term + far_term) * stretch).astype(jnp.bfloat16)
        out[level, rest] = upright(y)
        return y

    for block in range(blocks):
        settle(0, block, 1.0)
    zcross[0] = zrow[0]
    cross(0).start()
    gather(0)
    send(0, 0, 0)
    send(0, 1, 0)

    far_copy().wait_recv()
    y_rest = near_far(0, (0, 0))
    part[1] = project(rest, padded(y_rest[:kh], 0))
    part[2] = project(rest, padded(y_rest[kh:], 1))

    @arrivals(0, 0)
    def _(i):
        y = joined(0, 0, i)
        landed(0, 0, i)[...] = y
        part[1] += project(span(i), padded(y, 0))

    reduce(1, 1.0 / stretch)
    gather(1)
    send(1, 0, 1)

    @arrivals(0, 1)
    def _(i):
        y = joined(0, 1, i)
        part[2] += project(span(i), padded(y, 1))
        out[0, span(i)] = upright(jnp.concatenate([landed(0, 0, i)[...], y], axis=0))

    reduce(2, 1.0 / stretch)
    zcross[1] = zrow[1] + zrow[2]
    cross(1).start()
    gather(2)
    send(1, 1, 2)

    @arrivals(1, 0)
    def _(i):
        landed(1, 0, i)[...] = joined(1, 0, i)

    near_far(1, (1, 2))

    @arrivals(1, 1)
    def _(i):
        y = joined(1, 1, i)
        out[1, span(i)] = upright(jnp.concatenate([landed(1, 0, i)[...], y], axis=0))

    far_copy().wait_send()

    for stage in range(ITERS + 1):
        for buffer, send_sem, recv_sem in ((slot, rsend, rrecv), (zall, gsend, grecv)):
            peers = buffer.at[stage, :, pl.ds(1, cols - 1)]
            pltpu.make_async_remote_copy(
                src_ref=peers, dst_ref=peers,
                send_sem=send_sem.at[stage], recv_sem=recv_sem.at[stage, 0],
                device_id={"row": other}, device_id_type=MESH,
            ).wait_send()

    for level in range(ITERS):
        each(zallfar, (level,), hsend, hrecv).wait_send()
        cross(level).wait_send()

    for i in range(2):
        departure(i).wait_send()


def paired_body(matrix, probes):
    rows, width = matrix.shape
    k = probes.shape[1]
    kh = k // HALVES
    cols = lax.axis_size("col")
    stretch = math.sqrt(width * cols / (rows * lax.axis_size("row")))
    chunk = CHUNK
    tile = TILE
    spare = SPARE
    steps = (width - spare - 1) // tile
    last = width - spare - steps * tile
    blocks = rows // cols // LINES
    stages = ITERS + 1
    dma = pltpu.SemaphoreType.DMA
    return pl.pallas_call(
        functools.partial(kernel, stretch, cols, chunk, tile, spare),
        out_shape=pltpu.VMEM((ITERS, width, k), jnp.bfloat16),
        in_specs=[pl.BlockSpec(memory_space=pl.ANY)] * 2,
        out_specs=pl.BlockSpec(memory_space=pltpu.VMEM),
        scratch_shapes=[
            pltpu.VMEM((rows, width), jnp.bfloat16),
            pltpu.VMEM((width, k), jnp.bfloat16),
            pltpu.VMEM((ITERS, HALVES, steps, kh, tile), jnp.bfloat16),
            pltpu.VMEM((ITERS, HALVES, steps, kh, tile), jnp.bfloat16),
            pltpu.VMEM((ITERS, HALVES, kh, last), jnp.bfloat16),
            pltpu.VMEM((ITERS, HALVES, kh, last), jnp.bfloat16),
            pltpu.VMEM((stages, rows, k), jnp.float32),
            pltpu.VMEM((stages, blocks, cols, LINES, k), jnp.float32),
            pltpu.VMEM((stages, blocks, LINES, k), jnp.bfloat16),
            pltpu.VMEM((stages, blocks, cols, LINES, k), jnp.bfloat16),
            pltpu.VMEM((stages, k, rows), jnp.bfloat16),
            pltpu.VMEM((rows, spare), jnp.bfloat16),
            pltpu.VMEM((ITERS, blocks, LINES, k), jnp.bfloat16),
            pltpu.VMEM((ITERS, blocks, LINES, k), jnp.bfloat16),
            pltpu.VMEM((ITERS, cols, blocks, LINES, k), jnp.bfloat16),
            dma((width // chunk + (blocks - 1) * (width // (WIDER * chunk)),)),
            dma((width // chunk,)),
            dma((2,)),
            dma((ITERS, HALVES, steps // math.gcd(steps, GROUP) + 1)),
            dma((stages,)),
            dma((stages, blocks)),
            dma((stages,)),
            dma((stages, blocks)),
            dma,
            dma,
            dma((ITERS,)),
            dma((ITERS,)),
            dma((ITERS,)),
            dma((ITERS,)),
        ],
        compiler_params=pltpu.CompilerParams(
            vmem_limit_bytes=46 * 2**20, collective_id=0, has_side_effects=True
        ),
    )(matrix, probes)


def solution(mesh):
    placed = (P("row", "col"), P("col", None))
    body = paired_body if mesh.shape["row"] == 2 else plain_body
    return jax.shard_map(
        body, mesh=mesh, in_specs=placed, out_specs=P(None, "col", None), check_vma=False
    )
```

```python
import functools
import math

import jax
import jax.numpy as jnp
from jax import lax
from jax.experimental import pallas as pl
from jax.experimental.pallas import tpu as pltpu
from jax.sharding import PartitionSpec as P

ITERS = 2
HALVES = 2
CHUNK = 2048
LINES = 16
WIDER = 4
GROUP = 7
TILE = 1024
SPARE = 1024
MESH = pl.DeviceIdType.MESH


def plain_body(matrix, probes):
    m_total = matrix.shape[0] * lax.axis_size("row")
    n_total = matrix.shape[1] * lax.axis_size("col")
    stretch = math.sqrt(n_total / m_total)
    current = probes
    results = []
    for level in range(ITERS):
        factor = 1.0 if level == 0 else 1.0 / stretch
        partial_value = jnp.dot(matrix, current, preferred_element_type=jnp.float32)
        summed = lax.psum(partial_value, "col")
        reduced = (summed * factor).astype(jnp.bfloat16)
        whole_term = lax.dot_general(
            matrix, reduced, (((0,), (0,)), ((), ())), preferred_element_type=jnp.float32
        )
        portion = lax.psum_scatter(whole_term, "row", scatter_dimension=0, tiled=True)
        current = lax.all_gather(
            (portion * stretch).astype(jnp.bfloat16), "row", axis=0, tiled=True
        )
        results.append(current)
    return jnp.stack(results)


def kernel(
    stretch, cols, chunk, tile, spare,
    a_hbm, x_hbm, out,
    a, x, own, got, own_last, got_last, part, slot, zrow, zall, ztall, far, zcross, zfar, zallfar,
    a_sem, x_sem, psend, precv, rsend, rrecv, gsend, grecv,
    fsend, frecv, zsend, zrecv, hsend, hrecv,
):
    rows, width = a.shape
    k = x.shape[1]
    kh = k // HALVES
    main = width - spare
    steps = (main - 1) // tile
    last = main - steps * tile
    group = math.gcd(steps, GROUP)
    groups = steps // group
    owners = cols // 2
    band = owners * LINES
    blocks = rows // band
    mine = lax.axis_index("col")
    other = 1 - lax.axis_index("row")
    base = cols // 4
    rank = mine - base
    owner = (rank >= 0) & (rank < owners)

    def cut(block):
        return chunk if block == 0 else WIDER * chunk

    def load(block, i):
        return pl.ds(pl.multiple_of(i * cut(block), cut(block)), cut(block))

    def lines(block):
        return pl.ds(block * band, band)

    def span(i):
        if i is None:
            return pl.ds(steps * tile, last)
        return pl.ds(pl.multiple_of(i * tile, tile), tile)

    def sent(level, half, i):
        return own_last.at[level, half] if i is None else own.at[level, half, i]

    def landed(level, half, i):
        return got_last.at[level, half] if i is None else got.at[level, half, i]

    def tiles(body):
        pl.loop(0, steps)(body)
        body(None)

    def arrivals(level, half):
        def run(body):
            @pl.loop(0, groups)
            def _(g):
                arrival(level, half, g).wait_recv()
                pl.loop(g * group, (g + 1) * group)(body)

            swap(level, half, None).wait_recv()
            body(None)

        return run

    rest = pl.ds(main, spare)

    def a_copy(block, i):
        where = (lines(block), load(block, i))
        first = 0 if block == 0 else width // chunk + (block - 1) * (width // cut(1))
        return pltpu.make_async_copy(a_hbm.at[where], a.at[where], a_sem.at[first + i])

    def x_copy(i):
        where = load(0, i)
        return pltpu.make_async_copy(x_hbm.at[where], x.at[where], x_sem.at[i])

    def swap(level, half, i):
        return pltpu.make_async_remote_copy(
            src_ref=sent(level, half, i), dst_ref=landed(level, half, i),
            send_sem=psend.at[0 if i is not None else 1],
            recv_sem=precv.at[level, half, groups if i is None else i // group],
            device_id={"row": other}, device_id_type=MESH,
        )

    def arrival(level, half, g):
        members = (level, half, pl.ds(g * group, group))
        return pltpu.make_async_remote_copy(
            src_ref=own.at[members], dst_ref=got.at[members],
            send_sem=psend.at[0], recv_sem=precv.at[level, half, g],
            device_id={"row": other}, device_id_type=MESH,
        )

    def departure(i):
        return pltpu.make_async_remote_copy(
            src_ref=(own, own_last)[i], dst_ref=(got, got_last)[i],
            send_sem=psend.at[i], recv_sem=precv.at[0, 0, 0],
            device_id={"row": other}, device_id_type=MESH,
        )

    def each(buffer, where, count, send_sem, recv_sem):
        peers = buffer.at[(*where, pl.ds(0, count))]
        return pltpu.make_async_remote_copy(
            src_ref=peers, dst_ref=peers,
            send_sem=send_sem.at[where[0]], recv_sem=recv_sem.at[where],
            device_id={"col": lax.rem(mine + 1, cols)}, device_id_type=MESH,
        )

    def partner(code):
        if cols & (cols - 1):
            return lax.rem(mine + code, cols)
        peer, bit = 0, 1
        while bit < cols:
            digit = lax.rem(mine // bit, 2)
            peer += bit * (1 - digit if code & bit else digit)
            bit *= 2
        return peer

    codes = range(cols - 1, 0, -1)

    def piece(block, i):
        return pl.ds(pl.multiple_of(block * band + i * LINES, LINES), LINES)

    def scatter(stage, block, off):
        to = lax.rem(mine + cols - base + off, owners)
        return pltpu.make_async_remote_copy(
            src_ref=part.at[stage, piece(block, to)], dst_ref=slot.at[stage, block, mine],
            send_sem=rsend.at[stage], recv_sem=rrecv.at[stage, block],
            device_id={"col": base + to}, device_id_type=MESH,
        )

    def spread(stage, block, code):
        return pltpu.make_async_remote_copy(
            src_ref=zrow.at[stage, block], dst_ref=zall.at[stage, block, rank],
            send_sem=gsend.at[stage], recv_sem=grecv.at[stage, block],
            device_id={"col": partner(code)}, device_id_type=MESH,
        )

    def far_copy():
        return pltpu.make_async_remote_copy(
            src_ref=a_hbm.at[:, rest], dst_ref=far,
            send_sem=fsend, recv_sem=frecv,
            device_id={"row": other}, device_id_type=MESH,
        )

    def cross(level):
        return pltpu.make_async_remote_copy(
            src_ref=zcross.at[level], dst_ref=zfar.at[level],
            send_sem=zsend.at[level], recv_sem=zrecv.at[level],
            device_id={"row": other}, device_id_type=MESH,
        )

    def spread_far(level, code):
        return pltpu.make_async_remote_copy(
            src_ref=zfar.at[level], dst_ref=zallfar.at[level, rank],
            send_sem=hsend.at[level], recv_sem=hrecv.at[level],
            device_id={"col": partner(code)}, device_id_type=MESH,
        )

    def fetch(block, first, past):
        @pl.loop(first, past)
        def _(i):
            if block == 0:
                x_copy(i).start()
            a_copy(block, i).start()

    whole = width // chunk
    ahead = whole // 2
    fetch(0, 0, ahead)

    barrier = pltpu.get_barrier_semaphore()
    leader = cols - 1
    pl.semaphore_signal(barrier, inc=1, device_id={"row": other}, device_id_type=MESH)

    @pl.when(mine != leader)
    def _():
        pl.semaphore_wait(barrier, 1)
        far_copy().start()
        pl.semaphore_signal(barrier, inc=1, device_id={"col": leader}, device_id_type=MESH)

    fetch(0, ahead, whole)
    for block in range(1, blocks):
        fetch(block, 0, width // cut(block))

    part[0] = jnp.zeros((rows, k), jnp.float32)

    def first_product(block):
        def step(i):
            if block == 0:
                x_copy(i).wait()
            a_copy(block, i).wait()
            where = load(block, i)
            part[0, lines(block)] += jnp.dot(
                a[lines(block), where], x[where], preferred_element_type=jnp.float32
            )

        return step

    def scatters(stage, block):
        pl.when(~owner)(lambda: scatter(stage, block, 0).start())
        for off in range(1, owners):
            scatter(stage, block, off).start()

    def settle(stage, block, factor):
        @pl.when(owner)
        def _():
            each(slot, (stage, block), cols - 1, rsend, rrecv).wait_recv()
            slot[stage, block, mine] = part[stage, piece(block, rank)]
            acc = slot[stage, block, 0]
            for source in range(1, cols):
                acc += slot[stage, block, source]
            zrow[stage, block] = (acc * factor).astype(jnp.bfloat16)
            for code in codes:
                spread(stage, block, code).start()

    def collect(buffer, where, kept, send_sem, recv_sem):
        @pl.when(owner)
        def _():
            each(buffer, where, owners - 1, send_sem, recv_sem).wait_recv()
            buffer[(*where, rank)] = kept[where]

        @pl.when(~owner)
        def _():
            each(buffer, where, owners, send_sem, recv_sem).wait_recv()

    def across(pieces):
        return pieces.astype(jnp.float32).reshape(band, k).T.astype(jnp.bfloat16)

    def gather(stage):
        for block in range(blocks):
            collect(zall, (stage, block), zrow, gsend, grecv)
            ztall[stage, :, lines(block)] = across(zall[stage, block, :owners])

    def meet(level, rows_of):
        @pl.when(owner)
        def _():
            zcross[level] = rows_of()
            cross(level).start()

    def reduce(stage, factor):
        for block in range(blocks):
            scatters(stage, block)
        for block in range(blocks):
            settle(stage, block, factor)

    half_way = width // chunk // 2
    pl.loop(0, half_way)(first_product(0))

    @pl.when(mine == leader)
    def _():
        pl.semaphore_wait(barrier, cols)
        far_copy().start()

        @pl.loop(1, cols)
        def _(off):
            pl.semaphore_signal(
                barrier, inc=1, device_id={"col": lax.rem(mine + off, cols)}, device_id_type=MESH
            )

    pl.loop(half_way, width // chunk)(first_product(0))

    @pl.when(mine != leader)
    def _():
        pl.semaphore_wait(barrier, 1)

    scatters(0, 0)
    for block in range(1, blocks):
        pl.loop(0, width // cut(block))(first_product(block))
        scatters(0, block)

    def send(level, half, stage):
        kept = slice(half * kh, (half + 1) * kh)

        @tiles
        def _(i):
            term = jnp.dot(
                ztall[stage, kept], a[:, span(i)], preferred_element_type=jnp.float32
            )
            sent(level, half, i)[...] = (term * stretch).astype(jnp.bfloat16)
            swap(level, half, i).start()

    def joined(level, half, i):
        near = sent(level, half, i)[...].astype(jnp.float32)
        both = near + landed(level, half, i)[...].astype(jnp.float32)
        return both.astype(jnp.bfloat16)

    def padded(y, half):
        blank = jnp.zeros_like(y)
        return jnp.concatenate([y, blank] if half == 0 else [blank, y], axis=0)

    def project(where, y):
        return lax.dot_general(
            a[:, where], y, (((1,), (1,)), ((), ())), preferred_element_type=jnp.float32
        )

    def upright(y):
        return y.astype(jnp.float32).T.astype(jnp.bfloat16)

    def near_far(level, stages):
        @pl.when(owner)
        def _():
            cross(level).wait_recv()
            for code in codes:
                spread_far(level, code).start()

        collect(zallfar, (level,), zfar, hsend, hrecv)
        z_far = jnp.concatenate(
            [across(zallfar[level, :owners, block]) for block in range(blocks)], axis=1
        )
        z = jnp.concatenate(
            [ztall[s, h * kh:(h + 1) * kh] for h, s in enumerate(stages)], axis=0
        )
        near_term = jnp.dot(z, a[:, rest], preferred_element_type=jnp.float32)
        far_term = jnp.dot(z_far, far[...], preferred_element_type=jnp.float32)
        y = ((near_term + far_term) * stretch).astype(jnp.bfloat16)
        out[level, rest] = upright(y)
        return y

    for block in range(blocks):
        settle(0, block, 1.0)
    meet(0, lambda: zrow[0])
    gather(0)
    send(0, 0, 0)
    send(0, 1, 0)

    far_copy().wait_recv()
    y_rest = near_far(0, (0, 0))
    part[1] = project(rest, padded(y_rest[:kh], 0))
    part[2] = project(rest, padded(y_rest[kh:], 1))

    @arrivals(0, 0)
    def _(i):
        y = joined(0, 0, i)
        landed(0, 0, i)[...] = y
        part[1] += project(span(i), padded(y, 0))

    reduce(1, 1.0 / stretch)
    gather(1)
    send(1, 0, 1)

    @arrivals(0, 1)
    def _(i):
        y = joined(0, 1, i)
        part[2] += project(span(i), padded(y, 1))
        out[0, span(i)] = upright(jnp.concatenate([landed(0, 0, i)[...], y], axis=0))

    reduce(2, 1.0 / stretch)
    meet(1, lambda: zrow[1] + zrow[2])
    gather(2)
    send(1, 1, 2)

    @arrivals(1, 0)
    def _(i):
        landed(1, 0, i)[...] = joined(1, 0, i)

    near_far(1, (1, 2))

    @arrivals(1, 1)
    def _(i):
        y = joined(1, 1, i)
        out[1, span(i)] = upright(jnp.concatenate([landed(1, 0, i)[...], y], axis=0))

    far_copy().wait_send()

    def sent_all(buffer, stage, count, send_sem, recv_sem):
        peers = buffer.at[stage, :, pl.ds(0, count)]
        pltpu.make_async_remote_copy(
            src_ref=peers, dst_ref=peers,
            send_sem=send_sem.at[stage], recv_sem=recv_sem.at[stage, 0],
            device_id={"row": other}, device_id_type=MESH,
        ).wait_send()

    @pl.when(owner)
    def _():
        for stage in range(ITERS + 1):
            sent_all(slot, stage, owners - 1, rsend, rrecv)
            sent_all(zall, stage, cols - 1, gsend, grecv)
        for level in range(ITERS):
            each(zallfar, (level,), cols - 1, hsend, hrecv).wait_send()
            cross(level).wait_send()

    @pl.when(~owner)
    def _():
        for stage in range(ITERS + 1):
            sent_all(slot, stage, owners, rsend, rrecv)

    for i in range(2):
        departure(i).wait_send()


def paired_body(matrix, probes):
    rows, width = matrix.shape
    k = probes.shape[1]
    kh = k // HALVES
    cols = lax.axis_size("col")
    stretch = math.sqrt(width * cols / (rows * lax.axis_size("row")))
    chunk = CHUNK
    tile = TILE
    spare = SPARE
    steps = (width - spare - 1) // tile
    last = width - spare - steps * tile
    owners = cols // 2
    blocks = rows // (owners * LINES)
    stages = ITERS + 1
    dma = pltpu.SemaphoreType.DMA
    return pl.pallas_call(
        functools.partial(kernel, stretch, cols, chunk, tile, spare),
        out_shape=pltpu.VMEM((ITERS, width, k), jnp.bfloat16),
        in_specs=[pl.BlockSpec(memory_space=pl.ANY)] * 2,
        out_specs=pl.BlockSpec(memory_space=pltpu.VMEM),
        scratch_shapes=[
            pltpu.VMEM((rows, width), jnp.bfloat16),
            pltpu.VMEM((width, k), jnp.bfloat16),
            pltpu.VMEM((ITERS, HALVES, steps, kh, tile), jnp.bfloat16),
            pltpu.VMEM((ITERS, HALVES, steps, kh, tile), jnp.bfloat16),
            pltpu.VMEM((ITERS, HALVES, kh, last), jnp.bfloat16),
            pltpu.VMEM((ITERS, HALVES, kh, last), jnp.bfloat16),
            pltpu.VMEM((stages, rows, k), jnp.float32),
            pltpu.VMEM((stages, blocks, cols, LINES, k), jnp.float32),
            pltpu.VMEM((stages, blocks, LINES, k), jnp.bfloat16),
            pltpu.VMEM((stages, blocks, cols, LINES, k), jnp.bfloat16),
            pltpu.VMEM((stages, k, rows), jnp.bfloat16),
            pltpu.VMEM((rows, spare), jnp.bfloat16),
            pltpu.VMEM((ITERS, blocks, LINES, k), jnp.bfloat16),
            pltpu.VMEM((ITERS, blocks, LINES, k), jnp.bfloat16),
            pltpu.VMEM((ITERS, cols, blocks, LINES, k), jnp.bfloat16),
            dma((width // chunk + (blocks - 1) * (width // (WIDER * chunk)),)),
            dma((width // chunk,)),
            dma((2,)),
            dma((ITERS, HALVES, steps // math.gcd(steps, GROUP) + 1)),
            dma((stages,)),
            dma((stages, blocks)),
            dma((stages,)),
            dma((stages, blocks)),
            dma,
            dma,
            dma((ITERS,)),
            dma((ITERS,)),
            dma((ITERS,)),
            dma((ITERS,)),
        ],
        compiler_params=pltpu.CompilerParams(
            vmem_limit_bytes=46 * 2**20, collective_id=0, has_side_effects=True
        ),
    )(matrix, probes)


def solution(mesh):
    placed = (P("row", "col"), P("col", None))
    body = paired_body if mesh.shape["row"] == 2 else plain_body
    return jax.shard_map(
        body, mesh=mesh, in_specs=placed, out_specs=P(None, "col", None), check_vma=False
    )
```

```python
import functools
import math

import jax
import jax.numpy as jnp
from jax import lax
from jax.experimental import pallas as pl
from jax.experimental.pallas import tpu as pltpu
from jax.sharding import PartitionSpec as P

ITERS = 2
HALVES = 2
CHUNK = 2048
LINES = 8
WIDER = 4
GROUP = 14
TILE = 1024
SPARE = 1024
MESH = pl.DeviceIdType.MESH


def plain_body(matrix, probes):
    m_total = matrix.shape[0] * lax.axis_size("row")
    n_total = matrix.shape[1] * lax.axis_size("col")
    stretch = math.sqrt(n_total / m_total)
    current = probes
    results = []
    for level in range(ITERS):
        factor = 1.0 if level == 0 else 1.0 / stretch
        partial_value = jnp.dot(matrix, current, preferred_element_type=jnp.float32)
        summed = lax.psum(partial_value, "col")
        reduced = (summed * factor).astype(jnp.bfloat16)
        whole_term = lax.dot_general(
            matrix, reduced, (((0,), (0,)), ((), ())), preferred_element_type=jnp.float32
        )
        portion = lax.psum_scatter(whole_term, "row", scatter_dimension=0, tiled=True)
        current = lax.all_gather(
            (portion * stretch).astype(jnp.bfloat16), "row", axis=0, tiled=True
        )
        results.append(current)
    return jnp.stack(results)


def kernel(
    stretch, cols, chunk, tile, spare,
    a_hbm, x_hbm, out,
    a, x, own, got, own_last, got_last, part, slot, zrow, zall, ztall, far, zcross, zfar, zallfar,
    a_sem, x_sem, psend, precv, rsend, rrecv, gsend, grecv,
    fsend, frecv, zsend, zrecv, hsend, hrecv,
):
    rows, width = a.shape
    k = x.shape[1]
    kh = k // HALVES
    main = width - spare
    steps = (main - 1) // tile
    last = main - steps * tile
    group = math.gcd(steps, GROUP)
    groups = steps // group
    share = rows // cols
    blocks = share // LINES
    band = rows // blocks
    mine = lax.axis_index("col")
    other = 1 - lax.axis_index("row")

    def cut(block):
        return chunk if block == 0 else WIDER * chunk

    def load(block, i):
        return pl.ds(pl.multiple_of(i * cut(block), cut(block)), cut(block))

    def lines(block):
        return pl.ds(block * band, band)

    def span(i):
        if i is None:
            return pl.ds(steps * tile, last)
        return pl.ds(pl.multiple_of(i * tile, tile), tile)

    def sent(level, half, i):
        return own_last.at[level, half] if i is None else own.at[level, half, i]

    def landed(level, half, i):
        return got_last.at[level, half] if i is None else got.at[level, half, i]

    def tiles(body):
        pl.loop(0, steps)(body)
        body(None)

    def arrivals(level, half):
        def run(body):
            @pl.loop(0, groups)
            def _(g):
                arrival(level, half, g).wait_recv()
                pl.loop(g * group, (g + 1) * group)(body)

            swap(level, half, None).wait_recv()
            body(None)

        return run

    rest = pl.ds(main, spare)

    def a_copy(block, i):
        where = (lines(block), load(block, i))
        first = 0 if block == 0 else width // chunk + (block - 1) * (width // cut(1))
        return pltpu.make_async_copy(a_hbm.at[where], a.at[where], a_sem.at[first + i])

    def x_copy(i):
        where = load(0, i)
        return pltpu.make_async_copy(x_hbm.at[where], x.at[where], x_sem.at[i])

    def swap(level, half, i):
        return pltpu.make_async_remote_copy(
            src_ref=sent(level, half, i), dst_ref=landed(level, half, i),
            send_sem=psend.at[0 if i is not None else 1],
            recv_sem=precv.at[level, half, groups if i is None else i // group],
            device_id={"row": other}, device_id_type=MESH,
        )

    def arrival(level, half, g):
        members = (level, half, pl.ds(g * group, group))
        return pltpu.make_async_remote_copy(
            src_ref=own.at[members], dst_ref=got.at[members],
            send_sem=psend.at[0], recv_sem=precv.at[level, half, g],
            device_id={"row": other}, device_id_type=MESH,
        )

    def departure(i):
        return pltpu.make_async_remote_copy(
            src_ref=(own, own_last)[i], dst_ref=(got, got_last)[i],
            send_sem=psend.at[i], recv_sem=precv.at[0, 0, 0],
            device_id={"row": other}, device_id_type=MESH,
        )

    def each(buffer, where, send_sem, recv_sem):
        peers = buffer.at[(*where, pl.ds(1, cols - 1))]
        return pltpu.make_async_remote_copy(
            src_ref=peers, dst_ref=peers,
            send_sem=send_sem.at[where[0]], recv_sem=recv_sem.at[where],
            device_id={"col": lax.rem(mine + 1, cols)}, device_id_type=MESH,
        )

    def partner(code):
        if cols & (cols - 1):
            return lax.rem(mine + code, cols)
        peer, bit = 0, 1
        while bit < cols:
            digit = lax.rem(mine // bit, 2)
            peer += bit * (1 - digit if code & bit else digit)
            bit *= 2
        return peer

    codes = range(cols - 1, 0, -1)

    def piece(block, i):
        return pl.ds(pl.multiple_of(block * band + i * LINES, LINES), LINES)

    def scatter(stage, block, code):
        peer = partner(code)
        return pltpu.make_async_remote_copy(
            src_ref=part.at[stage, piece(block, peer)], dst_ref=slot.at[stage, block, code],
            send_sem=rsend.at[stage], recv_sem=rrecv.at[stage, block],
            device_id={"col": peer}, device_id_type=MESH,
        )

    def spread(stage, block, code):
        return pltpu.make_async_remote_copy(
            src_ref=zrow.at[stage, block], dst_ref=zall.at[stage, block, mine],
            send_sem=gsend.at[stage], recv_sem=grecv.at[stage, block],
            device_id={"col": partner(code)}, device_id_type=MESH,
        )

    def far_copy():
        return pltpu.make_async_remote_copy(
            src_ref=a_hbm.at[:, rest], dst_ref=far,
            send_sem=fsend, recv_sem=frecv,
            device_id={"row": other}, device_id_type=MESH,
        )

    def cross(level):
        return pltpu.make_async_remote_copy(
            src_ref=zcross.at[level], dst_ref=zfar.at[level],
            send_sem=zsend.at[level], recv_sem=zrecv.at[level],
            device_id={"row": other}, device_id_type=MESH,
        )

    def spread_far(level, code):
        return pltpu.make_async_remote_copy(
            src_ref=zfar.at[level], dst_ref=zallfar.at[level, mine],
            send_sem=hsend.at[level], recv_sem=hrecv.at[level],
            device_id={"col": partner(code)}, device_id_type=MESH,
        )

    barrier = pltpu.get_barrier_semaphore()
    pl.semaphore_signal(barrier, inc=1, device_id={"row": other}, device_id_type=MESH)

    def fetch(block, first, past):
        @pl.loop(first, past)
        def _(i):
            if block == 0:
                x_copy(i).start()
            a_copy(block, i).start()

    whole = width // chunk
    ahead = whole // 2
    fetch(0, 0, ahead)

    leader = 3 * cols // 4 - 1

    @pl.when(mine != leader)
    def _():
        pl.semaphore_wait(barrier, 1)
        far_copy().start()
        pl.semaphore_signal(barrier, inc=1, device_id={"col": leader}, device_id_type=MESH)

    fetch(0, ahead, whole)
    for block in range(1, blocks):
        fetch(block, 0, width // cut(block))

    part[0] = jnp.zeros((rows, k), jnp.float32)

    def first_product(block):
        def step(i):
            if block == 0:
                x_copy(i).wait()
            a_copy(block, i).wait()
            where = load(block, i)
            part[0, lines(block)] += jnp.dot(
                a[lines(block), where], x[where], preferred_element_type=jnp.float32
            )

        return step

    def scatters(stage, block):
        for code in codes:
            scatter(stage, block, code).start()

    def settle(stage, block, factor):
        each(slot, (stage, block), rsend, rrecv).wait_recv()
        acc = part[stage, piece(block, mine)]
        for code in codes:
            acc += slot[stage, block, code]
        zrow[stage, block] = (acc * factor).astype(jnp.bfloat16)
        for code in codes:
            spread(stage, block, code).start()

    def across(pieces):
        return pieces.astype(jnp.float32).reshape(band, k).T.astype(jnp.bfloat16)

    def gather(stage):
        for block in range(blocks):
            each(zall, (stage, block), gsend, grecv).wait_recv()
            zall[stage, block, mine] = zrow[stage, block]
            ztall[stage, :, lines(block)] = across(zall[stage, block])

    def reduce(stage, factor):
        for block in range(blocks):
            scatters(stage, block)
        for block in range(blocks):
            settle(stage, block, factor)

    half_way = width // chunk // 2
    pl.loop(0, half_way)(first_product(0))

    @pl.when(mine == leader)
    def _():
        pl.semaphore_wait(barrier, cols)
        far_copy().start()

        @pl.loop(1, cols)
        def _(off):
            pl.semaphore_signal(
                barrier, inc=1, device_id={"col": lax.rem(mine + off, cols)}, device_id_type=MESH
            )

    pl.loop(half_way, width // chunk)(first_product(0))

    @pl.when(mine != leader)
    def _():
        pl.semaphore_wait(barrier, 1)

    scatters(0, 0)
    for block in range(1, blocks):
        pl.loop(0, width // cut(block))(first_product(block))
        scatters(0, block)

    def send(level, half, stage):
        kept = slice(half * kh, (half + 1) * kh)

        @tiles
        def _(i):
            term = jnp.dot(
                ztall[stage, kept], a[:, span(i)], preferred_element_type=jnp.float32
            )
            sent(level, half, i)[...] = (term * stretch).astype(jnp.bfloat16)
            swap(level, half, i).start()

    def joined(level, half, i):
        near = sent(level, half, i)[...].astype(jnp.float32)
        both = near + landed(level, half, i)[...].astype(jnp.float32)
        return both.astype(jnp.bfloat16)

    def padded(y, half):
        blank = jnp.zeros_like(y)
        return jnp.concatenate([y, blank] if half == 0 else [blank, y], axis=0)

    def project(where, y):
        return lax.dot_general(
            a[:, where], y, (((1,), (1,)), ((), ())), preferred_element_type=jnp.float32
        )

    def upright(y):
        return y.astype(jnp.float32).T.astype(jnp.bfloat16)

    def near_far(level, stages):
        cross(level).wait_recv()

        for off in codes:
            spread_far(level, off).start()

        each(zallfar, (level,), hsend, hrecv).wait_recv()
        zallfar[level, mine] = zfar[level]
        z_far = jnp.concatenate(
            [across(zallfar[level, :, block]) for block in range(blocks)], axis=1
        )
        z = jnp.concatenate(
            [ztall[s, h * kh:(h + 1) * kh] for h, s in enumerate(stages)], axis=0
        )
        near_term = jnp.dot(z, a[:, rest], preferred_element_type=jnp.float32)
        far_term = jnp.dot(z_far, far[...], preferred_element_type=jnp.float32)
        y = ((near_term + far_term) * stretch).astype(jnp.bfloat16)
        out[level, rest] = upright(y)
        return y

    for block in range(blocks):
        settle(0, block, 1.0)
    zcross[0] = zrow[0]
    cross(0).start()
    gather(0)
    send(0, 0, 0)
    send(0, 1, 0)

    far_copy().wait_recv()
    y_rest = near_far(0, (0, 0))
    part[1] = project(rest, padded(y_rest[:kh], 0))
    part[2] = project(rest, padded(y_rest[kh:], 1))

    @arrivals(0, 0)
    def _(i):
        y = joined(0, 0, i)
        landed(0, 0, i)[...] = y
        part[1] += project(span(i), padded(y, 0))

    reduce(1, 1.0 / stretch)
    gather(1)
    send(1, 0, 1)

    @arrivals(0, 1)
    def _(i):
        y = joined(0, 1, i)
        part[2] += project(span(i), padded(y, 1))
        out[0, span(i)] = upright(jnp.concatenate([landed(0, 0, i)[...], y], axis=0))

    reduce(2, 1.0 / stretch)
    zcross[1] = zrow[1] + zrow[2]
    cross(1).start()
    gather(2)
    send(1, 1, 2)

    @arrivals(1, 0)
    def _(i):
        landed(1, 0, i)[...] = joined(1, 0, i)

    near_far(1, (1, 2))

    @arrivals(1, 1)
    def _(i):
        y = joined(1, 1, i)
        out[1, span(i)] = upright(jnp.concatenate([landed(1, 0, i)[...], y], axis=0))

    far_copy().wait_send()

    for stage in range(ITERS + 1):
        for buffer, send_sem, recv_sem in ((slot, rsend, rrecv), (zall, gsend, grecv)):
            peers = buffer.at[stage, :, pl.ds(1, cols - 1)]
            pltpu.make_async_remote_copy(
                src_ref=peers, dst_ref=peers,
                send_sem=send_sem.at[stage], recv_sem=recv_sem.at[stage, 0],
                device_id={"row": other}, device_id_type=MESH,
            ).wait_send()

    for level in range(ITERS):
        each(zallfar, (level,), hsend, hrecv).wait_send()
        cross(level).wait_send()

    for i in range(2):
        departure(i).wait_send()


def paired_body(matrix, probes):
    rows, width = matrix.shape
    k = probes.shape[1]
    kh = k // HALVES
    cols = lax.axis_size("col")
    stretch = math.sqrt(width * cols / (rows * lax.axis_size("row")))
    chunk = CHUNK
    tile = TILE
    spare = SPARE
    steps = (width - spare - 1) // tile
    last = width - spare - steps * tile
    blocks = rows // cols // LINES
    stages = ITERS + 1
    dma = pltpu.SemaphoreType.DMA
    return pl.pallas_call(
        functools.partial(kernel, stretch, cols, chunk, tile, spare),
        out_shape=pltpu.VMEM((ITERS, width, k), jnp.bfloat16),
        in_specs=[pl.BlockSpec(memory_space=pl.ANY)] * 2,
        out_specs=pl.BlockSpec(memory_space=pltpu.VMEM),
        scratch_shapes=[
            pltpu.VMEM((rows, width), jnp.bfloat16),
            pltpu.VMEM((width, k), jnp.bfloat16),
            pltpu.VMEM((ITERS, HALVES, steps, kh, tile), jnp.bfloat16),
            pltpu.VMEM((ITERS, HALVES, steps, kh, tile), jnp.bfloat16),
            pltpu.VMEM((ITERS, HALVES, kh, last), jnp.bfloat16),
            pltpu.VMEM((ITERS, HALVES, kh, last), jnp.bfloat16),
            pltpu.VMEM((stages, rows, k), jnp.float32),
            pltpu.VMEM((stages, blocks, cols, LINES, k), jnp.float32),
            pltpu.VMEM((stages, blocks, LINES, k), jnp.bfloat16),
            pltpu.VMEM((stages, blocks, cols, LINES, k), jnp.bfloat16),
            pltpu.VMEM((stages, k, rows), jnp.bfloat16),
            pltpu.VMEM((rows, spare), jnp.bfloat16),
            pltpu.VMEM((ITERS, blocks, LINES, k), jnp.bfloat16),
            pltpu.VMEM((ITERS, blocks, LINES, k), jnp.bfloat16),
            pltpu.VMEM((ITERS, cols, blocks, LINES, k), jnp.bfloat16),
            dma((width // chunk + (blocks - 1) * (width // (WIDER * chunk)),)),
            dma((width // chunk,)),
            dma((2,)),
            dma((ITERS, HALVES, steps // math.gcd(steps, GROUP) + 1)),
            dma((stages,)),
            dma((stages, blocks)),
            dma((stages,)),
            dma((stages, blocks)),
            dma,
            dma,
            dma((ITERS,)),
            dma((ITERS,)),
            dma((ITERS,)),
            dma((ITERS,)),
        ],
        compiler_params=pltpu.CompilerParams(
            vmem_limit_bytes=46 * 2**20, collective_id=0, has_side_effects=True
        ),
    )(matrix, probes)


def solution(mesh):
    placed = (P("row", "col"), P("col", None))
    body = paired_body if mesh.shape["row"] == 2 else plain_body
    return jax.shard_map(
        body, mesh=mesh, in_specs=placed, out_specs=P(None, "col", None), check_vma=False
    )
```
